32 devices in a mesh: farcp: 4 (over x, core), nearcp: 4 (over z), heads: 2 (over y).
Axes of the slice: x: 2, y: 2, z: 4, core: 2. Of those that a mesh axis runs over, the one named last changes fastest.
Arguments:
- raw_keys: bfloat16 [16, 24576, 8, 128], P(None, ('farcp', 'nearcp'), 'heads'), may hold values from -6 to 6
- raw_values: bfloat16 [16, 24576, 8, 128], P(None, ('farcp', 'nearcp'), 'heads'), may hold values from -6 to 6
- turn_angle: float32 [24576, 64], replicated, may hold values from -3.140625 to 3.140625
Outputs:
- stored_keys: bfloat16 [16, 8, 128, 24576], P(('farcp', 'nearcp'), 'heads')
- stored_values: bfloat16 [16, 24576, 8, 128], P(('farcp', 'nearcp'), None, 'heads')
- page_high: bfloat16 [16, 384, 8, 128], P(('farcp', 'nearcp'), None, 'heads')
- page_low: bfloat16 [16, 384, 8, 128], P(('farcp', 'nearcp'), None, 'heads')
The draws below stay inside these ranges and needn't reach their ends.
All inputs are finite; a program needn't handle non-finite values.
Results may differ from the reference program's by a relative error of at most 0.001.
Values may be sent and summed in bfloat16 or wider, within the bound.
A program may use at most 256 MiB of HBM per device.

```python
import jax
import jax.numpy as jnp

BATCH = 16
LENGTH = 24576
KV_HEADS = 8
HEAD_SIZE = 128
HALF_HEAD = 64
PAGE = 64


def shard_levels(own_key, dims, cuts, smallest, high):
    def one(dim, blocks):
        steps = jax.random.uniform(jax.random.fold_in(jax.random.fold_in(own_key, 6), dim), (blocks,), jnp.float32, smallest / len(cuts), high / len(cuts))
        return jnp.repeat(jnp.exp(steps), dims[dim] // blocks).reshape((-1,) + (1,) * (len(dims) - dim - 1))

    gain = one(*cuts[0])
    for cut in cuts[1:]:
        gain = gain * one(*cut)
    return gain


def bell_draw(rng, extent, width, reach, pieces=(), kind=jnp.bfloat16):
    gain = shard_levels(rng, extent, pieces, -0.22, 0.18) if pieces else 1.0
    array = jax.random.normal(rng, extent, jnp.float32) * width * gain
    return jnp.minimum(jnp.maximum(array, -reach), reach).astype(kind)


def setup_inputs(seed: int = 0) -> dict:
    key_of = jax.random.split(jax.random.key(seed), 4)
    return {
        "raw_keys": bell_draw(key_of[0], (BATCH, LENGTH, KV_HEADS, HEAD_SIZE), 1.0, 6.0, ((1, 16), (2, 2))),
        "raw_values": bell_draw(key_of[1], (BATCH, LENGTH, KV_HEADS, HEAD_SIZE), 1.0, 6.0, ((1, 16), (2, 2))),
        "turn_angle": jnp.clip(jax.random.uniform(key_of[2], (LENGTH, HALF_HEAD), jnp.float32, -3.140625, 3.140625), -3.140625, 3.140625),
    }


def apply_rotary(vectors, angle):
    half = vectors.shape[-1] // 2
    cosine, sine = jnp.cos(angle)[None, :, None, :], jnp.sin(angle)[None, :, None, :]
    first, second = vectors[..., :half], vectors[..., half:]
    return jnp.concatenate([first * cosine - second * sine, second * cosine + first * sine], axis=-1)


def keys_in_place(plain_keys, angle):
    wide_keys = plain_keys.astype(jnp.float32)
    return apply_rotary(wide_keys, angle)


def reference(raw_keys, raw_values, turn_angle):
    turned_keys = keys_in_place(raw_keys, turn_angle)
    narrow_keys = turned_keys.astype(jnp.bfloat16)
    page_view = narrow_keys.reshape(BATCH, LENGTH // PAGE, PAGE, KV_HEADS, HEAD_SIZE)
    page_high = jnp.max(page_view, axis=2)
    page_low = jnp.min(page_view, axis=2)
    stored_keys = jnp.transpose(narrow_keys, (0, 2, 3, 1))
    stored_values = raw_values
    return stored_keys, stored_values, page_high, page_low
```

```python
import functools

import jax
import jax.numpy as jnp
from jax import lax
from jax.experimental import pallas as pl
from jax.experimental.pallas import tpu as pltpu
from jax.sharding import PartitionSpec as P

PAGE = 64
AXES = ("farcp", "nearcp")
BLOCK = 256


def apply_rotary(vectors, angle):
    half = vectors.shape[-1] // 2
    cosine, sine = (jnp.cos(angle)[None, :, None, :], jnp.sin(angle)[None, :, None, :])
    first, second = (vectors[..., :half], vectors[..., half:])
    return jnp.concatenate(
        [first * cosine - second * sine, second * cosine + first * sine], axis=-1
    )


def exchange(array):
    return lax.all_to_all(array, AXES, split_axis=0, concat_axis=0, tiled=True)


def finish_kernel(heads, size, chunk_ref, *refs):
    keys_ref, high_ref, low_ref = refs[-3:]
    rows = chunk_ref.shape[1]
    for head in range(heads):
        part = chunk_ref[0, :, head * size : (head + 1) * size]
        keys_ref[0, head] = part.T
        for page in range(rows // PAGE):
            piece = part[page * PAGE : (page + 1) * PAGE]
            high_ref[0, page, head : head + 1, :] = jnp.max(piece, axis=0, keepdims=True)
            low_ref[0, page, head : head + 1, :] = jnp.min(piece, axis=0, keepdims=True)


def finish(chunk, before, start, span, heads, size):
    sources, rows, lanes = chunk.shape
    length = sources * span
    steps = rows // BLOCK
    where = lambda s, b: s * (span // BLOCK) + start // BLOCK + b
    outs = (
        jax.ShapeDtypeStruct((1, heads, size, length), chunk.dtype),
        jax.ShapeDtypeStruct((1, length // PAGE, heads, size), chunk.dtype),
        jax.ShapeDtypeStruct((1, length // PAGE, heads, size), chunk.dtype),
    )
    page_spec = pl.BlockSpec(
        (1, BLOCK // PAGE, heads, size), lambda s, b: (0, where(s, b), 0, 0)
    )
    in_specs = [pl.BlockSpec((1, BLOCK, lanes), lambda s, b: (s, b, 0))]
    in_specs += [pl.BlockSpec(memory_space=pl.ANY)] * len(before)
    return pl.pallas_call(
        functools.partial(finish_kernel, heads, size),
        grid=(sources, steps),
        in_specs=in_specs,
        out_specs=(
            pl.BlockSpec((1, heads, size, BLOCK), lambda s, b: (0, 0, 0, where(s, b))),
            page_spec,
            page_spec,
        ),
        out_shape=outs,
        input_output_aliases={1 + i: i for i in range(len(before))},
        cost_estimate=pl.CostEstimate(
            flops=4 * chunk.size, bytes_accessed=4 * chunk.size, transcendentals=0
        ),
        name=f"finish_{start}",
    )(chunk, *before)


def place_kernel(from_ref, to_ref):
    to_ref[...] = from_ref[...]


def place(array):
    spec = pl.BlockSpec((1,) + array.shape[1:], lambda s: (s, 0, 0, 0))
    return pl.pallas_call(
        place_kernel,
        grid=(array.shape[0],),
        in_specs=[spec],
        out_specs=spec,
        out_shape=jax.ShapeDtypeStruct(array.shape, array.dtype),
        cost_estimate=pl.CostEstimate(
            flops=0, bytes_accessed=4 * array.size, transcendentals=0
        ),
        name="place",
    )(array)


def per_device(raw_keys, raw_values, turn_angle):
    batch, span, heads, size = raw_keys.shape
    moved_values = exchange(raw_values)
    my_angles = lax.dynamic_slice_in_dim(turn_angle, lax.axis_index(AXES) * span, span)
    turned = apply_rotary(raw_keys.astype(jnp.float32), my_angles).astype(jnp.bfloat16)
    turned = turned.reshape(batch, span, heads * size)
    cut = span - BLOCK
    bounds = [(0, cut), (cut, span)] if cut else [(0, span)]
    pieces = [turned[:, first:last] for first, last in bounds]
    pieces, moved_values = lax.optimization_barrier((pieces, moved_values))
    arrived = exchange(pieces[0])
    stored_values = place(moved_values)
    done = finish(arrived, (), 0, span, heads, size)
    if cut:
        last, _, stored_values = lax.optimization_barrier((pieces[1], arrived, stored_values))
        done = finish(exchange(last), done, cut, span, heads, size)
    stored_values = stored_values.reshape(1, -1, heads, size)
    return (done[0], stored_values, done[1], done[2])


def solution(mesh):
    return jax.shard_map(
        per_device,
        mesh=mesh,
        in_specs=(
            P(None, AXES, "heads", None),
            P(None, AXES, "heads", None),
            P(),
        ),
        out_specs=(
            P(AXES, "heads", None, None),
            P(AXES, None, "heads", None),
            P(AXES, None, "heads", None),
            P(AXES, None, "heads", None),
        ),
        check_vma=False,
    )
```
